32 devices in a mesh: row: 4 (over y, x), col: 8 (over z, core).
Axes of the slice: x: 2, y: 2, z: 4, core: 2. Of those that a mesh axis runs over, the one named last changes fastest.
Arguments:
- matrix: float32 [2, 4, 256, 1, 8, 256], P(None, 'row', None, None, 'col'), as said below
Outputs:
- factored: float32 [2, 4, 256, 1, 8, 256], P(None, 'row', None, None, 'col')
Inputs may be any that keep to these rules, and one draw needn't show every extreme that they name: `matrix`: symmetric and positive definite.
All inputs are finite; a program needn't handle non-finite values.
Results may differ from the reference program's by a relative error of at most 0.0001.
Values sent between devices are 32-bit elements; how exact they have to be, the bound alone decides.
A program may use at most 128 MiB of HBM per device.

```python
import jax
import jax.numpy as jnp
from jax import lax

B = 256
MR = 2
STEPS = 8
MC = 1
N_ROW = 4
N_COL = 8


def draw_matrix(key, part):
    order = MR * N_ROW * B
    inner_count = order // 4
    first, second = jax.random.split(key, 2)
    factor_g = jax.random.normal(first, (order, inner_count), jnp.float32)
    product = jnp.dot(factor_g, factor_g.T, precision=lax.Precision.HIGHEST, preferred_element_type=jnp.float32)
    product = product * (1.0 / inner_count)
    product = 0.5 * (product + product.T)
    diag_vals = jax.random.uniform(second, (order,), jnp.float32, 0.5, 1.5)
    result = product + jnp.diag(diag_vals)
    return result.reshape(MR, N_ROW, B, MC, N_COL, B)


def setup_inputs(seed: int = 0) -> dict:
    streams_of = jax.random.split(jax.random.key(seed), 2)
    return {
        "matrix": draw_matrix(jax.random.fold_in(streams_of[1], 71), 0),
    }


def reference(matrix):
    order = MR * N_ROW * B
    work = matrix.reshape(order, order)
    for k in range(STEPS):
        low = k * B
        high = low + B
        factor = jnp.linalg.cholesky(work[low:high, low:high])
        below = work[high:, low:high]
        solved = jax.scipy.linalg.solve_triangular(factor, below.T, lower=True).T
        update = jnp.dot(solved.astype(jnp.float32), solved.T.astype(jnp.float32), precision=lax.Precision.HIGHEST, preferred_element_type=jnp.float32)
        work = work.at[high:, high:].add(-update)
        work = work.at[:low, low:high].set(jnp.zeros((low, B), jnp.float32))
        work = work.at[low:high, low:high].set(factor)
        work = work.at[high:, low:high].set(solved)
    return work.reshape(matrix.shape)
```

```python
import functools

import jax
import jax.numpy as jnp
from jax import lax
from jax.experimental import pallas as pl
from jax.experimental.pallas import tpu as pltpu
from jax.sharding import PartitionSpec as P

STEPS = 8
LANES = 128
SUBS = 8
PANEL = 64
BLOCK = 16
SHAPE = (SUBS, LANES)
ROOT_COL = 2
MESH = pl.DeviceIdType.MESH
NT = (((1,), (1,)), ((), ()))
TN = (((0,), (0,)), ((), ()))


def split(value):
    high = value.astype(jnp.bfloat16)
    low = (value - high.astype(jnp.float32)).astype(jnp.bfloat16)
    return high, low


def dot3(a_high, a_low, b_high, b_low):
    def one(a, b):
        return lax.dot_general(a, b, NT, preferred_element_type=jnp.float32)

    return one(a_high, b_high) + (one(a_high, b_low) + one(a_low, b_high))


def spread(value, at):
    return jnp.broadcast_to(value[at:at+1,:], SHAPE)

def factor_panel(work, diag, unit, width, start):
    groups = PANEL//SUBS
    chunks = width//LANES
    sub = lax.broadcasted_iota(jnp.int32, SHAPE, 0)
    lane = lax.broadcasted_iota(jnp.int32, SHAPE, 1)
    rows = [[work[start+g*SUBS:start+(g+1)*SUBS, h*LANES:(h+1)*LANES] for h in range(chunks)] for g in range(groups)]
    per = BLOCK//SUBS
    for b in range(PANEL//BLOCK):
        home = b*per
        l0 = start + b*BLOCK
        hc, off = l0//LANES, l0%LANES
        def pick(g, t):
            return jnp.take_along_axis(rows[g][hc], jnp.full(SHAPE, off+t, jnp.int32), axis=1)
        near = min(home+2*per, groups)
        far = list(range(near, groups))
        cols = [{g: pick(g,t) for g in range(home + t//SUBS, near)} for t in range(BLOCK)]
        fcols = [{g: pick(g,t) for g in far} for t in range(SUBS)] + [{}]*SUBS
        scales = {g: jnp.ones(SHAPE, jnp.float32) for g in range(home, home+per)}
        lower = {g: jnp.zeros(SHAPE, jnp.float32) for g in range(home, home+per)}
        for t in range(0, BLOCK, 2):
            top = home + t//SUBS
            r = t%SUBS
            if t == SUBS and far:
                fcols = [None]*SUBS + [{g: pick(g,SUBS+q) for g in far} for q in range(SUBS)]
            if r == 0:
                inside = jnp.logical_and(lane>=off+t, lane<off+t+SUBS)
                eye = jnp.where(lane == off+t+sub, unit[hc], 0.0)
                for g in range(top, groups):
                    rows[g][hc] = jnp.where(inside, eye if g == top else 0.0, rows[g][hc])
            x, y = dict(cols[t]), dict(cols[t+1])
            fx, fy = fcols[t], fcols[t+1]
            a, bb, c = spread(x[top], r), spread(x[top], r+1), spread(y[top], r+1)
            det = a*c - bb*bb
            ra = lax.rsqrt(a)
            rd = lax.rsqrt(a*det)
            ia, iad = ra*ra, rd*rd
            u = {g: y[g]*a - x[g]*bb for g in y}
            fu = {g: fy[g]*a - fx[g]*bb for g in far}
            mx = {g: x[g]*ia for g in x}
            mu = {g: u[g]*iad for g in u}
            fmx = {g: fx[g]*ia for g in far}
            fmu = {g: fu[g]*iad for g in far}
            for s in range(t+2, BLOCK):
                gs, q = home + s//SUBS, s%SUBS
                xs, us = spread(x[gs], q), spread(u[gs], q)
                for g in cols[s]:
                    if s < t+4 and g == gs:
                        cols[s][g] = (cols[s][g] - xs*mx[g]) - (us*u[g])*iad
                    else:
                        cols[s][g] = cols[s][g] - xs*mx[g] - us*mu[g]
                if s < SUBS or t >= SUBS:
                    for g in far:
                        fcols[s][g] = fcols[s][g] - xs*fmx[g] - us*fmu[g]
            for g in [top]:
                lower[g] = jnp.where(lane==off+t, x[g]*ra, jnp.where(lane==off+t+1, u[g]*rd, lower[g]))
            scales[top] = jnp.where(sub==r, ra, jnp.where(sub==r+1, a*rd, scales[top]))
            mx[top] = jnp.where(sub>r, mx[top], 0.0)
            mu[top] = jnp.where(sub>r+1, mu[top], 0.0)
            for h in range(chunks):
                p0, q1 = spread(rows[top][h], r), spread(rows[top][h], r+1)
                p1 = q1*a - p0*bb
                for g in range(top, groups):
                    m, n = (fmx[g], fmu[g]) if g in far else (mx[g], mu[g])
                    rows[g][h] = rows[g][h] - m*p0 - n*p1
            if r == SUBS-2:
                rows[top] = [v*scales[top] for v in rows[top]]
        for g in range(home, home+per):
            diag[start+g*SUBS:start+(g+1)*SUBS, :] = lower[g]
    for g in range(groups):
        for h in range(chunks):
            work[start+g*SUBS:start+(g+1)*SUBS, h*LANES:(h+1)*LANES] = rows[g][h]
    stop = start+PANEL
    if stop == width: return
    hc = start//LANES
    for g in range(groups):
        gap = jnp.logical_and(lane>=start%LANES+(g+1)*SUBS, lane<start%LANES+PANEL)
        rows[g][hc] = jnp.where(gap, 0.0, rows[g][hc])
    whole = jnp.concatenate([jnp.concatenate(r,1) for r in rows],0)
    high, low = split(whole)
    base = stop//LANES*LANES
    lh, ll = high[:, base:], low[:, base:]
    update = lax.dot_general(jnp.concatenate([lh,lh,ll],0), jnp.concatenate([high,low,high],0), TN, preferred_element_type=jnp.float32)
    lanes = lax.broadcasted_iota(jnp.int32, (width-stop, width), 1)
    old = jnp.where(jnp.logical_and(lanes >= start, lanes < stop), 0.0, work[stop:, :])
    work[stop:, :] = old - update[stop-base:, :]

def factor_tile(work, diag, scale_row, width):
    chunks = width//LANES
    unit = [jnp.broadcast_to(scale_row[:, h*LANES:(h+1)*LANES], SHAPE) for h in range(chunks)]
    for start in range(0, width, PANEL):
        factor_panel(work, diag, unit, width, start)


def kernel(dims, x_ref, o_ref, tiles, high, low, work, corner, inv_high, inv_low, in_sem, out_sem, send_sem, land_sem, go_sem):
    steps, num_row, num_col = dims
    row_tiles, width, _ = x_ref.shape
    my_row, my_col = lax.axis_index("row"), lax.axis_index("col")
    root_row, root_col = num_row - 1, min(ROOT_COL, num_col - 1)
    home = (root_row, root_col)
    root = jnp.logical_and(my_row == root_row, my_col == root_col)
    count = num_row * num_col
    barrier = pltpu.get_barrier_semaphore()

    def inbound(a, i, slot, device):
        return pltpu.make_async_remote_copy(
            src_ref=x_ref.at[a], dst_ref=tiles.at[slot], send_sem=send_sem.at[a], recv_sem=in_sem.at[slot],
            device_id=device, device_id_type=MESH,
        )

    def outbound(slot, a, device):
        return pltpu.make_async_remote_copy(
            src_ref=tiles.at[slot], dst_ref=o_ref.at[a], send_sem=out_sem.at[slot], recv_sem=land_sem.at[a],
            device_id=device, device_id_type=MESH,
        )

    beside = my_row == root_row
    ahead = jnp.where(jnp.logical_and(beside, my_col - 1 == root_col), my_col - 2, my_col - 1)
    after = jnp.where(jnp.logical_and(beside, my_col + 1 == root_col), my_col + 2, my_col + 1)
    follows, leads = ahead >= 0, after < num_col

    @pl.when(jnp.logical_not(root))
    def _():
        pl.semaphore_signal(barrier, inc=1, device_id=home, device_id_type=MESH)

        @pl.when(follows)
        def _():
            pl.semaphore_signal(barrier, inc=1, device_id=(my_row, ahead), device_id_type=MESH)

        pl.semaphore_wait(barrier, jnp.where(leads, 2, 1))

        @pl.when(follows)
        def _():
            pl.semaphore_wait(go_sem, 1)

        for a in range(row_tiles):
            i = a * num_row + my_row

            @pl.when(i >= my_col)
            def _():
                inbound(a, i, i * steps + my_col, home).start()

            @pl.when(i < my_col)
            def _():
                o_ref[a] = jnp.zeros((width, width), jnp.float32)

        for a in range(row_tiles):
            i = a * num_row + my_row

            @pl.when(i >= my_col)
            def _():
                inbound(a, i, i * steps + my_col, home).wait_send()

        @pl.when(leads)
        def _():
            pl.semaphore_signal(go_sem, inc=1, device_id=(my_row, after), device_id_type=MESH)

        for a in range(row_tiles):
            i = a * num_row + my_row

            @pl.when(i >= my_col)
            def _():
                outbound(0, a, home).wait_recv()

    @pl.when(root)
    def _():
        for a in range(row_tiles):
            i = a * num_row + root_row
            if i >= root_col:
                slot = i * steps + root_col
                pltpu.make_async_copy(x_ref.at[a], tiles.at[slot], in_sem.at[slot]).start()
            else:
                o_ref[a] = jnp.zeros((width, width), jnp.float32)

        def greet(d, carry):
            d = jnp.where(d >= root_row * num_col + root_col, d + 1, d)
            pl.semaphore_signal(
                barrier, inc=1, device_id=(d // num_col, lax.rem(d, num_col)), device_id_type=MESH
            )
            return carry

        lax.fori_loop(0, count - 1, greet, 0)
        pl.semaphore_wait(barrier, count - 1)

        def arrive(slot):
            pltpu.make_async_copy(tiles.at[slot], tiles.at[slot], in_sem.at[slot]).wait()

        def owned(i, k):
            return jnp.logical_and(lax.rem(i, num_row) == root_row, k == root_col)

        def send(i, k):
            slot = i * steps + k

            @pl.when(owned(i, k))
            def _():
                pltpu.make_async_copy(tiles.at[slot], o_ref.at[i // num_row], out_sem.at[slot]).start()

            @pl.when(jnp.logical_not(owned(i, k)))
            def _():
                outbound(slot, i // num_row, (lax.rem(i, num_row), k)).start()

        def block(i):
            return pl.ds(pl.multiple_of(i * width, width), width)

        def subtract(i, k):
            slot = i * steps + k
            arrive(slot)

            def one(m, carry):
                tiles[slot] -= dot3(
                    high[block(i), block(m)], low[block(i), block(m)],
                    high[block(k), block(m)], low[block(k), block(m)],
                )
                return carry

            lax.fori_loop(0, k, one, 0)

        def step(k, carry):
            slot = k * steps + k
            subtract(k, k)
            rows = lax.broadcasted_iota(jnp.int32, (width, width), 0)
            cols = lax.broadcasted_iota(jnp.int32, (width, width), 1)
            tile = tiles[slot]
            only = jnp.where(rows == cols, tile, 0.0)
            along = jnp.sum(only, axis=0, keepdims=True)
            down = jnp.sum(only, axis=1, keepdims=True)
            scale_row, scale_col = lax.rsqrt(along), lax.rsqrt(down)
            work[...] = tile * scale_row * scale_col
            factor_tile(work, corner, scale_row, width)
            done = work[...]
            inv_high[...], inv_low[...] = split(jnp.where(cols <= rows, done, 0.0))
            upper = jnp.where(cols // SUBS > rows // SUBS, done * (along * scale_row), 0.0)
            wide = jnp.concatenate([corner[...]] * (width // LANES), 1)
            near = jnp.logical_and(cols // SUBS == rows // SUBS, cols <= rows)
            tiles[slot] = upper.T + jnp.where(near, wide * (down * scale_col), 0.0)

            def panel(i, carry):
                send(i - 1, k)
                subtract(i, k)
                spot = i * steps + k
                a_high, a_low = split(tiles[spot])
                solved = dot3(a_high, a_low, inv_high[...], inv_low[...])
                tiles[spot] = solved
                high[block(i), block(k)], low[block(i), block(k)] = split(solved)
                return carry

            lax.fori_loop(k + 1, steps, panel, 0)

            send(steps - 1, k)
            return carry

        lax.fori_loop(0, steps, step, 0)

        def finish(k, carry):
            def one(i, carry):
                slot = i * steps + k
                pltpu.make_async_copy(tiles.at[slot], tiles.at[slot], out_sem.at[slot]).wait()
                return carry

            return lax.fori_loop(k, steps, one, carry)

        lax.fori_loop(0, steps, finish, 0)


def on_root(matrix):
    row_tiles = matrix.shape[0]
    width = matrix.shape[2]
    num_row, num_col = lax.axis_size("row"), lax.axis_size("col")
    order = STEPS * width
    local = matrix.reshape(row_tiles, width, width)
    slots = STEPS * STEPS
    out = pl.pallas_call(
        functools.partial(kernel, (STEPS, num_row, num_col)),
        out_shape=jax.ShapeDtypeStruct(local.shape, jnp.float32),
        in_specs=[pl.BlockSpec(memory_space=pltpu.VMEM)],
        out_specs=pl.BlockSpec(memory_space=pltpu.VMEM),
        scratch_shapes=[
            pltpu.VMEM((slots, width, width), jnp.float32),
            pltpu.VMEM((order, order), jnp.bfloat16),
            pltpu.VMEM((order, order), jnp.bfloat16),
            pltpu.VMEM((width, width), jnp.float32),
            pltpu.VMEM((width, LANES), jnp.float32),
            pltpu.VMEM((width, width), jnp.bfloat16),
            pltpu.VMEM((width, width), jnp.bfloat16),
            pltpu.SemaphoreType.DMA((slots,)),
            pltpu.SemaphoreType.DMA((slots,)),
            pltpu.SemaphoreType.DMA((row_tiles,)),
            pltpu.SemaphoreType.DMA((row_tiles,)),
            pltpu.SemaphoreType.REGULAR,
        ],
        compiler_params=pltpu.CompilerParams(collective_id=0, has_side_effects=True, vmem_limit_bytes=56 * 2**20),
    )(local)
    return out.reshape(matrix.shape)


def broadcast(value, axis, source):
    kept = jnp.where(lax.axis_index(axis) == source, value, 0).astype(value.dtype)
    return lax.psum(kept, axis)


def solve_panel(factor, column):
    width = column.shape[1]
    inverse = jax.scipy.linalg.solve_triangular(
        factor, jnp.eye(width, dtype=jnp.float32), lower=True
    )
    solved = jnp.einsum("ts,ars->art", inverse, column, precision=lax.Precision.HIGHEST)
    return solved


def stepwise(matrix):
    row_tiles = matrix.shape[0]
    width = matrix.shape[2]
    col_tiles = matrix.shape[3]
    tile_grid = matrix.reshape(row_tiles, width, col_tiles, width)
    num_row = lax.axis_size("row")
    num_col = lax.axis_size("col")
    my_row = lax.axis_index("row")
    my_col = lax.axis_index("col")
    rows_global = jnp.arange(row_tiles, dtype=jnp.int32) * num_row + my_row
    ratio = num_col // num_row
    for k in range(STEPS):
        lead_row = k % num_row
        lead_col = k % num_col
        local_row = k // num_row
        local_col = k // num_col
        column = tile_grid[:, :, local_col, :]
        candidate = tile_grid[local_row, :, local_col, :]
        keep = (rows_global > k)[:, None, None]
        diag_tile = broadcast(candidate, "row", lead_row)
        factor = jnp.linalg.cholesky(diag_tile)
        local_panel = jnp.where(keep, solve_panel(factor, column), 0.0)
        panel_rows = broadcast(local_panel, "col", lead_col)
        grouped = panel_rows.reshape(col_tiles, ratio, width, width)
        chosen = lax.dynamic_index_in_dim(grouped, my_col // num_row, 1, keepdims=False)
        panel_cols = broadcast(chosen, "row", my_col % num_row)
        update = jnp.einsum(
            "art,bst->arbs", panel_rows, panel_cols, precision=lax.Precision.HIGHEST
        )
        tile_grid = tile_grid - update
        diagonal_part = jnp.where((rows_global == k)[:, None, None], factor[None], 0.0)
        new_column = panel_rows + diagonal_part
        old_column = tile_grid[:, :, local_col, :]
        tile_grid = tile_grid.at[:, :, local_col, :].set(
            jnp.where(my_col == lead_col, new_column, old_column)
        )
    return tile_grid.reshape(matrix.shape)


def on_device(matrix):
    row_tiles, _, _, col_tiles = matrix.shape[:4]
    whole = row_tiles * lax.axis_size("row") == STEPS and lax.axis_size("col") == STEPS and col_tiles == 1
    return on_root(matrix) if whole else stepwise(matrix)


def solution(mesh):
    placed = (P(None, "row", None, None, "col", None),)
    return jax.shard_map(
        on_device,
        mesh=mesh,
        in_specs=placed,
        out_specs=P(None, "row", None, None, "col", None),
        check_vma=False,
    )
```

```python
import functools

import jax
import jax.numpy as jnp
from jax import lax
from jax.experimental import pallas as pl
from jax.experimental.pallas import tpu as pltpu
from jax.sharding import PartitionSpec as P

STEPS = 8
LANES = 128
SUBS = 8
PANEL = 64
BLOCK = 16
SHAPE = (SUBS, LANES)
MESH = pl.DeviceIdType.MESH
NT = (((1,), (1,)), ((), ()))
TN = (((0,), (0,)), ((), ()))


def split(value):
    high = value.astype(jnp.bfloat16)
    low = (value - high.astype(jnp.float32)).astype(jnp.bfloat16)
    return high, low


def dot3(a_high, a_low, b_high, b_low):
    def one(a, b):
        return lax.dot_general(a, b, NT, preferred_element_type=jnp.float32)

    return one(a_high, b_high) + (one(a_high, b_low) + one(a_low, b_high))


def spread(value, at):
    return jnp.broadcast_to(value[at:at+1,:], SHAPE)

def factor_panel(work, diag, unit, width, start):
    groups = PANEL//SUBS
    chunks = width//LANES
    sub = lax.broadcasted_iota(jnp.int32, SHAPE, 0)
    lane = lax.broadcasted_iota(jnp.int32, SHAPE, 1)
    rows = [[work[start+g*SUBS:start+(g+1)*SUBS, h*LANES:(h+1)*LANES] for h in range(chunks)] for g in range(groups)]
    per = BLOCK//SUBS
    for b in range(PANEL//BLOCK):
        home = b*per
        l0 = start + b*BLOCK
        hc, off = l0//LANES, l0%LANES
        def pick(g, t):
            return jnp.take_along_axis(rows[g][hc], jnp.full(SHAPE, off+t, jnp.int32), axis=1)
        near = min(home+2*per, groups)
        far = list(range(near, groups))
        cols = [{g: pick(g,t) for g in range(home + t//SUBS, near)} for t in range(BLOCK)]
        fcols = [{g: pick(g,t) for g in far} for t in range(SUBS)] + [{}]*SUBS
        scales = {g: jnp.ones(SHAPE, jnp.float32) for g in range(home, home+per)}
        lower = {g: jnp.zeros(SHAPE, jnp.float32) for g in range(home, home+per)}
        for t in range(0, BLOCK, 2):
            top = home + t//SUBS
            r = t%SUBS
            if t == SUBS and far:
                fcols = [None]*SUBS + [{g: pick(g,SUBS+q) for g in far} for q in range(SUBS)]
            if r == 0:
                inside = jnp.logical_and(lane>=off+t, lane<off+t+SUBS)
                eye = jnp.where(lane == off+t+sub, unit[hc], 0.0)
                for g in range(top, groups):
                    rows[g][hc] = jnp.where(inside, eye if g == top else 0.0, rows[g][hc])
            x, y = dict(cols[t]), dict(cols[t+1])
            fx, fy = fcols[t], fcols[t+1]
            a, bb, c = spread(x[top], r), spread(x[top], r+1), spread(y[top], r+1)
            det = a*c - bb*bb
            ra = lax.rsqrt(a)
            rd = lax.rsqrt(a*det)
            ia, iad = ra*ra, rd*rd
            u = {g: y[g]*a - x[g]*bb for g in y}
            fu = {g: fy[g]*a - fx[g]*bb for g in far}
            mx = {g: x[g]*ia for g in x}
            mu = {g: u[g]*iad for g in u}
            fmx = {g: fx[g]*ia for g in far}
            fmu = {g: fu[g]*iad for g in far}
            for s in range(t+2, BLOCK):
                gs, q = home + s//SUBS, s%SUBS
                xs, us = spread(x[gs], q), spread(u[gs], q)
                for g in cols[s]:
                    if s < t+4 and g == gs:
                        cols[s][g] = (cols[s][g] - xs*mx[g]) - (us*u[g])*iad
                    else:
                        cols[s][g] = cols[s][g] - xs*mx[g] - us*mu[g]
                if s < SUBS or t >= SUBS:
                    for g in far:
                        fcols[s][g] = fcols[s][g] - xs*fmx[g] - us*fmu[g]
            for g in [top]:
                lower[g] = jnp.where(lane==off+t, x[g]*ra, jnp.where(lane==off+t+1, u[g]*rd, lower[g]))
            scales[top] = jnp.where(sub==r, ra, jnp.where(sub==r+1, a*rd, scales[top]))
            mx[top] = jnp.where(sub>r, mx[top], 0.0)
            mu[top] = jnp.where(sub>r+1, mu[top], 0.0)
            for h in range(chunks):
                p0, q1 = spread(rows[top][h], r), spread(rows[top][h], r+1)
                p1 = q1*a - p0*bb
                for g in range(top, groups):
                    m, n = (fmx[g], fmu[g]) if g in far else (mx[g], mu[g])
                    rows[g][h] = rows[g][h] - m*p0 - n*p1
            if r == SUBS-2:
                rows[top] = [v*scales[top] for v in rows[top]]
        for g in range(home, home+per):
            diag[start+g*SUBS:start+(g+1)*SUBS, :] = lower[g]
    for g in range(groups):
        for h in range(chunks):
            work[start+g*SUBS:start+(g+1)*SUBS, h*LANES:(h+1)*LANES] = rows[g][h]
    stop = start+PANEL
    if stop == width: return
    hc = start//LANES
    for g in range(groups):
        gap = jnp.logical_and(lane>=start%LANES+(g+1)*SUBS, lane<start%LANES+PANEL)
        rows[g][hc] = jnp.where(gap, 0.0, rows[g][hc])
    whole = jnp.concatenate([jnp.concatenate(r,1) for r in rows],0)
    high, low = split(whole)
    base = stop//LANES*LANES
    lh, ll = high[:, base:], low[:, base:]
    update = lax.dot_general(jnp.concatenate([lh,lh,ll],0), jnp.concatenate([high,low,high],0), TN, preferred_element_type=jnp.float32)
    lanes = lax.broadcasted_iota(jnp.int32, (width-stop, width), 1)
    old = jnp.where(jnp.logical_and(lanes >= start, lanes < stop), 0.0, work[stop:, :])
    work[stop:, :] = old - update[stop-base:, :]

def factor_tile(work, diag, scale_row, width):
    chunks = width//LANES
    unit = [jnp.broadcast_to(scale_row[:, h*LANES:(h+1)*LANES], SHAPE) for h in range(chunks)]
    for start in range(0, width, PANEL):
        factor_panel(work, diag, unit, width, start)


def load(ref):
    half = ref.shape[0] // 2
    return jnp.concatenate([ref[pl.ds(h, half, stride=2), :] for h in range(2)], 1)


def store(ref, value):
    half = ref.shape[0] // 2
    for h in range(2):
        ref[pl.ds(h, half, stride=2), :] = value[:, h * LANES : (h + 1) * LANES]


def kernel(
    dims, x_ref, o_ref, tiles, inverse, beside, relay, high, low, own_high, own_low, inv_high, inv_low, work, corner,
    in_sem, out_sem, pass_sem, inv_in, inv_out, first_out, side_in, side_out, send_sem, land_sem, relay_in, relay_out,
    go_sem,
):
    steps, num_row, num_col = dims
    row_tiles = x_ref.shape[0]
    width = work.shape[0]
    my_row, my_col = lax.axis_index("row"), lax.axis_index("col")
    root_row = num_row - 1
    chief, helper = (root_row, 3), (root_row, 2)
    first = jnp.logical_and(my_row == 0, my_col == 0)
    is_chief = jnp.logical_and(my_row == chief[0], my_col == chief[1])
    is_helper = jnp.logical_and(my_row == helper[0], my_col == helper[1])
    count = num_row * num_col
    me = my_row * num_col + my_col
    barrier = pltpu.get_barrier_semaphore()
    far = jnp.logical_or(my_col < 2, my_col > 3)

    def remote(src, dst, send, recv, device):
        return pltpu.make_async_remote_copy(
            src_ref=src, dst_ref=dst, send_sem=send, recv_sem=recv, device_id=device, device_id_type=MESH
        )

    def local(src, dst, sem):
        return pltpu.make_async_copy(src, dst, sem)

    def settle(ref, sem):
        pltpu.make_async_copy(ref, ref, sem).wait()

    def own(a):
        return (a * num_row + my_row) * steps + my_col

    def to_chief(a):
        return remote(x_ref.at[a], tiles.at[own(a)], send_sem.at[a], in_sem.at[own(a)], chief)

    def to_helper(a):
        return remote(x_ref.at[a], tiles.at[own(a)], send_sem.at[a], in_sem.at[own(a)], helper)

    def to_relay(a):
        return remote(x_ref.at[a], relay.at[my_row], send_sem.at[a], relay_in.at[my_row], (root_row, my_col))

    def onward(p):
        slot = (num_row + p) * steps + my_col
        return remote(relay.at[p], tiles.at[slot], relay_out.at[p], in_sem.at[slot], helper)

    def signal(sem, device):
        pl.semaphore_signal(sem, inc=1, device_id=device, device_id_type=MESH)

    relayed = jnp.logical_and(far, jnp.logical_and(my_row < 2, num_row + my_row >= my_col))
    relays = [
        jnp.logical_and(jnp.logical_and(my_row == root_row, far), num_row + p >= my_col) for p in range(2)
    ]

    @pl.when(jnp.logical_not(is_chief))
    def _():
        signal(barrier, chief)

    @pl.when(jnp.logical_not(is_helper))
    def _():
        signal(barrier, helper)

    for p in range(2):

        @pl.when(relays[p])
        def _(p=p):
            signal(barrier, (p, my_col))

    @pl.when(jnp.logical_or(is_chief, is_helper))
    def _():
        def greet(d, carry):
            signal(barrier, (d // num_col, lax.rem(d, num_col)))
            return carry

        mine = chief[0] * num_col + jnp.where(is_chief, chief[1], helper[1])
        other = chief[0] * num_col + jnp.where(is_chief, helper[1], chief[1])
        low_end, high_end = jnp.minimum(mine, other), jnp.maximum(mine, other)
        lax.fori_loop(0, low_end, greet, 0)
        lax.fori_loop(high_end + 1, count, greet, 0)
        pl.semaphore_wait(barrier, count - 1)

    @pl.when(jnp.logical_not(jnp.logical_or(first, jnp.logical_or(is_chief, is_helper))))
    def _():
        pl.semaphore_wait(barrier, jnp.where(relayed, 3, 2))

    for a in range(row_tiles):

        @pl.when(a * num_row + my_row < my_col)
        def _(a=a):
            o_ref[a] = jnp.zeros(o_ref.shape[1:], jnp.float32)

    begin = jnp.logical_and(my_row == 1, my_col <= 1)

    @pl.when(begin)
    def _():
        to_chief(0).start()

    early = jnp.logical_and(jnp.logical_and(my_row >= 2, my_row >= my_col), jnp.logical_not(is_helper))

    @pl.when(early)
    def _():
        to_helper(0).start()

    @pl.when(is_helper)
    def _():
        for a in range(row_tiles):
            local(x_ref.at[a], tiles.at[own(a)], in_sem.at[own(a)]).start()

    @pl.when(jnp.logical_and(relayed, jnp.logical_not(first)))
    def _():
        to_relay(1).start()

    for p in range(2):

        @pl.when(relays[p])
        def _(p=p):
            settle(relay.at[p], relay_in.at[p])
            onward(p).start()

    last = num_row + my_row >= my_col
    late = jnp.logical_and(
        last, jnp.logical_or(my_row == 2, jnp.logical_and(my_row < 2, jnp.logical_not(far)))
    )

    @pl.when(late)
    def _():
        pl.semaphore_wait(go_sem, 1)

    end = jnp.logical_or(late, jnp.logical_and(my_row == root_row, jnp.logical_not(is_helper)))

    @pl.when(end)
    def _():
        to_helper(1).start()

    def arrive(slot):
        settle(tiles.at[slot], in_sem.at[slot])

    def deliver(slot, a, row, col):
        return remote(tiles.at[slot], o_ref.at[a], out_sem.at[slot], land_sem.at[a], (row, col))

    def send(i, k):
        slot = i * steps + k
        row, a = lax.rem(i, num_row), i // num_row
        home = jnp.logical_and(my_row == row, my_col == k)

        @pl.when(home)
        def _():
            local(tiles.at[slot], o_ref.at[a], out_sem.at[slot]).start()

        @pl.when(jnp.logical_not(home))
        def _():
            deliver(slot, a, row, k).start()

    def inv_copy(k, sem, device):
        return remote(inverse.at[k], inverse.at[k], sem, inv_in.at[k], device)

    def side_copy(k):
        return remote(tiles.at[(k + 1) * steps + k], beside.at[k], side_out.at[k], side_in.at[k], helper)

    @pl.when(first)
    def _():
        local(x_ref.at[0], tiles.at[0], in_sem.at[0]).start()

    @pl.when(jnp.logical_or(first, is_chief))
    def _():
        def step(k, carry):
            slot = k * steps + k

            @pl.when(is_chief)
            def _():
                @pl.when(k == 1)
                def _():
                    settle(inverse.at[0], inv_in.at[0])
                    inv_high[0], inv_low[0] = split(load(inverse.at[0]))

                left = slot - 1
                arrive(left)
                a_high, a_low = split(load(tiles.at[left]))
                solved = dot3(a_high, a_low, inv_high[0], inv_low[0])
                store(tiles.at[left], solved)
                own_high[...], own_low[...] = split(solved)

                @pl.when(k < steps - 1)
                def _():
                    side_copy(k - 1).start()

                send(k, k - 1)

            arrive(slot)

            @pl.when(k == 1)
            def _():
                for p in range(2):
                    for q in range(2, 4):
                        signal(go_sem, (p, q))

            work[...] = load(tiles.at[slot])

            @pl.when(is_chief)
            def _():
                work[...] -= dot3(own_high[...], own_low[...], own_high[...], own_low[...])

            rows = lax.broadcasted_iota(jnp.int32, (width, width), 0)
            cols = lax.broadcasted_iota(jnp.int32, (width, width), 1)
            tile = work[...]
            only = jnp.where(rows == cols, tile, 0.0)
            along = jnp.sum(only, axis=0, keepdims=True)
            down = jnp.sum(only, axis=1, keepdims=True)
            scale_row, scale_col = lax.rsqrt(along), lax.rsqrt(down)
            work[...] = tile * scale_row * scale_col
            factor_tile(work, corner, scale_row, width)

            @pl.when(k < steps - 1)
            def _():
                found = jnp.where(cols <= rows, work[...], 0.0)
                store(inverse.at[k], found)
                inv_high[0], inv_low[0] = split(found)

            @pl.when(first)
            def _():
                pl.semaphore_wait(barrier, 3)
                inv_copy(k, first_out.at[0], chief).start()
                inv_copy(k, first_out.at[1], helper).start()

            @pl.when(jnp.logical_and(is_chief, k < steps - 2))
            def _():
                inv_copy(k, inv_out.at[k], helper).start()

            upper = jnp.where(cols // SUBS > rows // SUBS, work[...] * (along * scale_row), 0.0)
            wide = jnp.concatenate([corner[...]] * (width // LANES), 1)
            near = jnp.logical_and(cols // SUBS == rows // SUBS, cols <= rows)
            store(tiles.at[slot], upper.T + jnp.where(near, wide * (down * scale_col), 0.0))
            send(k, k)
            return carry

        lax.fori_loop(jnp.where(first, 0, 1), jnp.where(first, 1, steps), step, 0)

    @pl.when(first)
    def _():
        to_relay(1).start()
        settle(tiles.at[0], out_sem.at[0])
        inv_copy(0, first_out.at[0], chief).wait_send()
        inv_copy(0, first_out.at[1], helper).wait_send()

    @pl.when(is_chief)
    def _():
        def finish(k, carry):
            settle(tiles.at[k * steps + k], out_sem.at[k * steps + k])
            settle(tiles.at[k * steps + k - 1], out_sem.at[k * steps + k - 1])

            @pl.when(k < steps - 1)
            def _():
                settle(beside.at[k - 1], side_out.at[k - 1])

            @pl.when(k < steps - 2)
            def _():
                settle(inverse.at[k], inv_out.at[k])

            return carry

        lax.fori_loop(1, steps, finish, 0)

    def block(i):
        return pl.ds(pl.multiple_of(i * width, width), width)

    @pl.when(is_helper)
    def _():
        def row(i, carry):
            def whole(j, carry):
                arrive(i * steps + j)
                return carry

            lax.fori_loop(0, i + 1, whole, 0)

            @pl.when(i == 2)
            def _():
                for q in range(num_col - 1):
                    signal(go_sem, (2, q))

            def stage(k, carry):
                @pl.when(k == i - 2)
                def _():
                    settle(inverse.at[k], inv_in.at[k])
                    inv_high[k], inv_low[k] = split(load(inverse.at[k]))
                    settle(beside.at[k], side_in.at[k])
                    high[block(k + 1), block(k)], low[block(k + 1), block(k)] = split(load(beside.at[k]))

                spot = i * steps + k
                a_high, a_low = split(load(tiles.at[spot]))
                solved = dot3(a_high, a_low, inv_high[k], inv_low[k])
                store(tiles.at[spot], solved)
                high[block(i), block(k)], low[block(i), block(k)] = split(solved)
                send(i, k)

                def one(j, carry):
                    slot = i * steps + j
                    update = dot3(
                        high[block(i), block(k)], low[block(i), block(k)],
                        high[block(j), block(k)], low[block(j), block(k)],
                    )
                    store(tiles.at[slot], load(tiles.at[slot]) - update)
                    return carry

                lax.fori_loop(k + 1, i + 1, one, 0)
                return carry

            lax.fori_loop(0, i - 1, stage, 0)
            for j in (i - 1, i):
                slot = i * steps + j
                remote(tiles.at[slot], tiles.at[slot], pass_sem.at[slot], in_sem.at[slot], chief).start()
            return carry

        lax.fori_loop(2, steps, row, 0)

        def finish(i, carry):
            def each(k, carry):
                settle(tiles.at[i * steps + k], out_sem.at[i * steps + k])
                return carry

            lax.fori_loop(0, i - 1, each, 0)
            for j in (i - 1, i):
                settle(tiles.at[i * steps + j], pass_sem.at[i * steps + j])
            return carry

        lax.fori_loop(2, steps, finish, 0)

    sent = [jnp.logical_or(begin, early), jnp.logical_or(relayed, end)]
    for a in range(row_tiles):

        @pl.when(sent[a])
        def _(a=a):
            to_helper(a).wait_send()

        i = a * num_row + my_row
        diagonal = jnp.logical_and(is_chief, i == my_col)
        below = jnp.logical_and(is_helper, i >= my_col + 2)
        mine = jnp.logical_or(jnp.logical_or(below, diagonal), jnp.logical_and(first, a == 0))

        @pl.when(jnp.logical_and(i >= my_col, jnp.logical_not(mine)))
        def _(a=a):
            settle(o_ref.at[a], land_sem.at[a])

    for p in range(2):

        @pl.when(relays[p])
        def _(p=p):
            onward(p).wait_send()


def on_root(matrix):
    row_tiles = matrix.shape[0]
    width = matrix.shape[2]
    num_row, num_col = lax.axis_size("row"), lax.axis_size("col")
    order = STEPS * width
    tall = width * width // LANES
    local = matrix.reshape(row_tiles, tall, LANES)
    slots = STEPS * STEPS
    sem = pltpu.SemaphoreType.DMA
    out = pl.pallas_call(
        functools.partial(kernel, (STEPS, num_row, num_col)),
        out_shape=jax.ShapeDtypeStruct(local.shape, jnp.float32),
        in_specs=[pl.BlockSpec(memory_space=pltpu.VMEM)],
        out_specs=pl.BlockSpec(memory_space=pltpu.VMEM),
        scratch_shapes=[
            pltpu.VMEM((slots, tall, LANES), jnp.float32),
            pltpu.VMEM((STEPS, tall, LANES), jnp.float32),
            pltpu.VMEM((STEPS, tall, LANES), jnp.float32),
            pltpu.VMEM((2, tall, LANES), jnp.float32),
            pltpu.VMEM((order, order), jnp.bfloat16),
            pltpu.VMEM((order, order), jnp.bfloat16),
            pltpu.VMEM((width, width), jnp.bfloat16),
            pltpu.VMEM((width, width), jnp.bfloat16),
            pltpu.VMEM((STEPS, width, width), jnp.bfloat16),
            pltpu.VMEM((STEPS, width, width), jnp.bfloat16),
            pltpu.VMEM((width, width), jnp.float32),
            pltpu.VMEM((width, LANES), jnp.float32),
            sem((slots,)), sem((slots,)), sem((slots,)), sem((STEPS,)), sem((STEPS,)), sem((2,)), sem((STEPS,)),
            sem((STEPS,)), sem((row_tiles,)), sem((row_tiles,)), sem((2,)), sem((2,)),
            pltpu.SemaphoreType.REGULAR,
        ],
        compiler_params=pltpu.CompilerParams(collective_id=0, has_side_effects=True, vmem_limit_bytes=56 * 2**20),
    )(local)
    return out.reshape(matrix.shape)


def broadcast(value, axis, source):
    kept = jnp.where(lax.axis_index(axis) == source, value, 0).astype(value.dtype)
    return lax.psum(kept, axis)


def solve_panel(factor, column):
    width = column.shape[1]
    inverse = jax.scipy.linalg.solve_triangular(
        factor, jnp.eye(width, dtype=jnp.float32), lower=True
    )
    solved = jnp.einsum("ts,ars->art", inverse, column, precision=lax.Precision.HIGHEST)
    return solved


def stepwise(matrix):
    row_tiles = matrix.shape[0]
    width = matrix.shape[2]
    col_tiles = matrix.shape[3]
    tile_grid = matrix.reshape(row_tiles, width, col_tiles, width)
    num_row = lax.axis_size("row")
    num_col = lax.axis_size("col")
    my_row = lax.axis_index("row")
    my_col = lax.axis_index("col")
    rows_global = jnp.arange(row_tiles, dtype=jnp.int32) * num_row + my_row
    ratio = num_col // num_row
    for k in range(STEPS):
        lead_row = k % num_row
        lead_col = k % num_col
        local_row = k // num_row
        local_col = k // num_col
        column = tile_grid[:, :, local_col, :]
        candidate = tile_grid[local_row, :, local_col, :]
        keep = (rows_global > k)[:, None, None]
        diag_tile = broadcast(candidate, "row", lead_row)
        factor = jnp.linalg.cholesky(diag_tile)
        local_panel = jnp.where(keep, solve_panel(factor, column), 0.0)
        panel_rows = broadcast(local_panel, "col", lead_col)
        grouped = panel_rows.reshape(col_tiles, ratio, width, width)
        chosen = lax.dynamic_index_in_dim(grouped, my_col // num_row, 1, keepdims=False)
        panel_cols = broadcast(chosen, "row", my_col % num_row)
        update = jnp.einsum(
            "art,bst->arbs", panel_rows, panel_cols, precision=lax.Precision.HIGHEST
        )
        tile_grid = tile_grid - update
        diagonal_part = jnp.where((rows_global == k)[:, None, None], factor[None], 0.0)
        new_column = panel_rows + diagonal_part
        old_column = tile_grid[:, :, local_col, :]
        tile_grid = tile_grid.at[:, :, local_col, :].set(
            jnp.where(my_col == lead_col, new_column, old_column)
        )
    return tile_grid.reshape(matrix.shape)


def on_device(matrix):
    row_tiles, _, _, col_tiles = matrix.shape[:4]
    whole = row_tiles == 2 and 2 * lax.axis_size("row") == STEPS and lax.axis_size("col") == STEPS and col_tiles == 1
    return on_root(matrix) if whole else stepwise(matrix)


def solution(mesh):
    placed = (P(None, "row", None, None, "col", None),)
    return jax.shard_map(
        on_device,
        mesh=mesh,
        in_specs=placed,
        out_specs=P(None, "row", None, None, "col", None),
        check_vma=False,
    )
```

```python
import functools

import jax
import jax.numpy as jnp
from jax import lax
from jax.experimental import pallas as pl
from jax.experimental.pallas import tpu as pltpu
from jax.sharding import PartitionSpec as P

STEPS = 8
LANES = 128
SUBS = 8
PANEL = 64
BLOCK = 16
SHAPE = (SUBS, LANES)
MESH = pl.DeviceIdType.MESH
PASSED = ((4, 0), (4, 1), (4, 4), (5, 4), (5, 5), (6, 5), (6, 6))
NT = (((1,), (1,)), ((), ()))
TN = (((0,), (0,)), ((), ()))


def split(value):
    high = value.astype(jnp.bfloat16)
    low = (value - high.astype(jnp.float32)).astype(jnp.bfloat16)
    return high, low


def dot3(a_high, a_low, b_high, b_low):
    def one(a, b):
        return lax.dot_general(a, b, NT, preferred_element_type=jnp.float32)

    return one(a_high, b_high) + (one(a_high, b_low) + one(a_low, b_high))


def spread(value, at):
    return jnp.broadcast_to(value[at:at+1,:], SHAPE)

def factor_panel(work, diag, unit, width, start, after):
    groups = PANEL//SUBS
    chunks = width//LANES
    sub = lax.broadcasted_iota(jnp.int32, SHAPE, 0)
    lane = lax.broadcasted_iota(jnp.int32, SHAPE, 1)
    rows = [[work[start+g*SUBS:start+(g+1)*SUBS, h*LANES:(h+1)*LANES] for h in range(chunks)] for g in range(groups)]
    per = BLOCK//SUBS
    for b in range(PANEL//BLOCK):
        home = b*per
        l0 = start + b*BLOCK
        hc, off = l0//LANES, l0%LANES
        def pick(g, t):
            return jnp.take_along_axis(rows[g][hc], jnp.full(SHAPE, off+t, jnp.int32), axis=1)
        near = min(home+2*per, groups)
        far = list(range(near, groups))
        cols = [{g: pick(g,t) for g in range(home + t//SUBS, near)} for t in range(BLOCK)]
        fcols = [{g: pick(g,t) for g in far} for t in range(SUBS)] + [{}]*SUBS
        scales = {g: jnp.ones(SHAPE, jnp.float32) for g in range(home, home+per)}
        lower = {g: jnp.zeros(SHAPE, jnp.float32) for g in range(home, home+per)}
        for t in range(0, BLOCK, 2):
            top = home + t//SUBS
            r = t%SUBS
            if t == SUBS and far:
                fcols = [None]*SUBS + [{g: pick(g,SUBS+q) for g in far} for q in range(SUBS)]
            if r == 0:
                inside = jnp.logical_and(lane>=off+t, lane<off+t+SUBS)
                eye = jnp.where(lane == off+t+sub, unit[hc], 0.0)
                for g in range(top, groups):
                    rows[g][hc] = jnp.where(inside, eye if g == top else 0.0, rows[g][hc])
            x, y = dict(cols[t]), dict(cols[t+1])
            fx, fy = fcols[t], fcols[t+1]
            a, bb, c = spread(x[top], r), spread(x[top], r+1), spread(y[top], r+1)
            det = a*c - bb*bb
            ra = lax.rsqrt(a)
            rd = lax.rsqrt(a*det)
            ia, iad = ra*ra, rd*rd
            u = {g: y[g]*a - x[g]*bb for g in y}
            fu = {g: fy[g]*a - fx[g]*bb for g in far}
            mx = {g: x[g]*ia for g in x}
            mu = {g: u[g]*iad for g in u}
            fmx = {g: fx[g]*ia for g in far}
            fmu = {g: fu[g]*iad for g in far}
            for s in range(t+2, BLOCK):
                gs, q = home + s//SUBS, s%SUBS
                xs, us = spread(x[gs], q), spread(u[gs], q)
                for g in cols[s]:
                    if s < t+4 and g == gs:
                        cols[s][g] = (cols[s][g] - xs*mx[g]) - (us*u[g])*iad
                    else:
                        cols[s][g] = cols[s][g] - xs*mx[g] - us*mu[g]
                if s < SUBS or t >= SUBS:
                    for g in far:
                        fcols[s][g] = fcols[s][g] - xs*fmx[g] - us*fmu[g]
            for g in [top]:
                lower[g] = jnp.where(lane==off+t, x[g]*ra, jnp.where(lane==off+t+1, u[g]*rd, lower[g]))
            scales[top] = jnp.where(sub==r, ra, jnp.where(sub==r+1, a*rd, scales[top]))
            mx[top] = jnp.where(sub>r, mx[top], 0.0)
            mu[top] = jnp.where(sub>r+1, mu[top], 0.0)
            for h in range(chunks):
                p0, q1 = spread(rows[top][h], r), spread(rows[top][h], r+1)
                p1 = q1*a - p0*bb
                for g in range(top, groups):
                    m, n = (fmx[g], fmu[g]) if g in far else (mx[g], mu[g])
                    rows[g][h] = rows[g][h] - m*p0 - n*p1
            if r == SUBS-2:
                rows[top] = [v*scales[top] for v in rows[top]]
        for g in range(home, home+per):
            diag[start+g*SUBS:start+(g+1)*SUBS, :] = lower[g]
    for g in range(groups):
        for h in range(chunks):
            work[start+g*SUBS:start+(g+1)*SUBS, h*LANES:(h+1)*LANES] = rows[g][h]
    stop = start+PANEL
    after(start)
    if stop == width: return
    hc = start//LANES
    for g in range(groups):
        gap = jnp.logical_and(lane>=start%LANES+(g+1)*SUBS, lane<start%LANES+PANEL)
        rows[g][hc] = jnp.where(gap, 0.0, rows[g][hc])
    whole = jnp.concatenate([jnp.concatenate(r,1) for r in rows],0)
    high, low = split(whole)
    base = stop//LANES*LANES
    lh, ll = high[:, base:], low[:, base:]
    update = lax.dot_general(jnp.concatenate([lh,lh,ll],0), jnp.concatenate([high,low,high],0), TN, preferred_element_type=jnp.float32)
    lanes = lax.broadcasted_iota(jnp.int32, (width-stop, width), 1)
    old = jnp.where(jnp.logical_and(lanes >= start, lanes < stop), 0.0, work[stop:, :])
    work[stop:, :] = old - update[stop-base:, :]

def factor_tile(work, diag, scale_row, width, after=lambda start: None):
    chunks = width//LANES
    unit = [jnp.broadcast_to(scale_row[:, h*LANES:(h+1)*LANES], SHAPE) for h in range(chunks)]
    for start in range(0, width, PANEL):
        factor_panel(work, diag, unit, width, start, after)


def load(ref):
    half = ref.shape[0] // 2
    return jnp.concatenate([ref[pl.ds(h, half, stride=2), :] for h in range(2)], 1)


def store(ref, value):
    half = ref.shape[0] // 2
    for h in range(2):
        ref[pl.ds(h, half, stride=2), :] = value[:, h * LANES : (h + 1) * LANES]


def kernel(
    dims, x_ref, o_ref, tiles, inverse, beside, relay, high, low, own_high, own_low, inv_high, inv_low, work, corner,
    in_sem, out_sem, pass_sem, inv_in, inv_out, first_in, first_out, side_in, side_out, send_sem, land_sem, relay_in, relay_out,
    half_sem, go_sem,
):
    steps, num_row, num_col = dims
    row_tiles = x_ref.shape[0]
    width = work.shape[0]
    my_row, my_col = lax.axis_index("row"), lax.axis_index("col")
    root_row = num_row - 1
    chief, helper = (root_row, 3), (root_row, 2)
    first = jnp.logical_and(my_row == 0, my_col == 0)
    is_chief = jnp.logical_and(my_row == chief[0], my_col == chief[1])
    is_helper = jnp.logical_and(my_row == helper[0], my_col == helper[1])
    count = num_row * num_col
    me = my_row * num_col + my_col
    barrier = pltpu.get_barrier_semaphore()
    far = jnp.logical_or(my_col < 2, my_col > 3)

    def remote(src, dst, send, recv, device):
        return pltpu.make_async_remote_copy(
            src_ref=src, dst_ref=dst, send_sem=send, recv_sem=recv, device_id=device, device_id_type=MESH
        )

    def local(src, dst, sem):
        return pltpu.make_async_copy(src, dst, sem)

    def settle(ref, sem):
        pltpu.make_async_copy(ref, ref, sem).wait()

    def own(a):
        return (a * num_row + my_row) * steps + my_col

    def to_chief(a):
        return remote(x_ref.at[a], tiles.at[own(a)], send_sem.at[a], in_sem.at[own(a)], chief)

    def to_helper(a):
        return remote(x_ref.at[a], tiles.at[own(a)], send_sem.at[a], in_sem.at[own(a)], helper)

    def to_relay(a):
        return remote(x_ref.at[a], relay.at[my_row], send_sem.at[a], relay_in.at[my_row], (root_row, my_col))

    def onward(p):
        slot = (num_row + p) * steps + my_col
        return remote(relay.at[p], tiles.at[slot], relay_out.at[p], in_sem.at[slot], helper)

    def signal(sem, device):
        pl.semaphore_signal(sem, inc=1, device_id=device, device_id_type=MESH)

    def via(i, j):
        return max(i % num_row, 1), 2 + j % 2

    def at(row, col):
        return jnp.logical_and(my_row == row, my_col == col)

    second = num_row + my_row >= my_col
    relayed = jnp.logical_and(jnp.logical_and(far, second), my_row < jnp.where(my_col > 3, 3, 2))
    at_relay = jnp.logical_and(my_row == root_row, far)
    relays = [jnp.logical_and(at_relay, num_row + p >= my_col) for p in range(2)]
    relays.append(jnp.logical_and(at_relay, jnp.logical_and(my_col > 3, num_row + 2 >= my_col)))

    @pl.when(jnp.logical_not(is_chief))
    def _():
        signal(barrier, chief)

    @pl.when(jnp.logical_not(is_helper))
    def _():
        signal(barrier, helper)

    for p in range(3):

        @pl.when(relays[p])
        def _(p=p):
            signal(barrier, (p, my_col))

    for i, j in PASSED:

        @pl.when(at(i % num_row, j))
        def _(i=i, j=j):
            signal(barrier, via(i, j))

    @pl.when(at(0, 1))
    def _():
        signal(barrier, (root_row, 1))

    @pl.when(jnp.logical_or(is_chief, is_helper))
    def _():
        def greet(d, carry):
            signal(barrier, (lax.rem(d, num_row), d // num_row))
            return carry

        low_end, high_end = helper[1] * num_row + helper[0], chief[1] * num_row + chief[0]
        lax.fori_loop(0, low_end, greet, 0)
        lax.fori_loop(low_end + 1, high_end, greet, 0)
        lax.fori_loop(high_end + 1, count, greet, 0)
        pl.semaphore_wait(barrier, count - 1)

    @pl.when(jnp.logical_not(jnp.logical_or(first, jnp.logical_or(is_chief, is_helper))))
    def _():
        expected = jnp.where(jnp.logical_or(relayed, at(root_row, 1)), 3, 2)
        for i, j in PASSED:
            expected += jnp.where(at(*via(i, j)), 1, 0)
        pl.semaphore_wait(barrier, expected)

    tall = x_ref.shape[1]
    corner_slot = steps + 1

    def half_in(p):
        span = pl.ds(p * (tall // 2), tall // 2)
        return remote(x_ref.at[0, span], relay.at[2, span], half_sem.at[0, p], half_sem.at[1, p], (root_row, 1))

    def half_on(p):
        span = pl.ds(p * (tall // 2), tall // 2)
        return remote(
            relay.at[2, span], tiles.at[corner_slot, span], half_sem.at[2, p], in_sem.at[corner_slot], chief
        )

    begin = at(1, 0)

    @pl.when(begin)
    def _():
        to_chief(0).start()
        to_chief(0).wait_send()

    @pl.when(at(1, 1))
    def _():
        for p in range(2):
            half_in(p).start()

    @pl.when(at(root_row, 1))
    def _():
        for p in range(2):
            half_in(p).wait_recv()
            half_on(p).start()
        signal(go_sem, (0, 1))

    @pl.when(at(0, 1))
    def _():
        pl.semaphore_wait(go_sem, 1)

    early = jnp.logical_and(jnp.logical_and(my_row >= 2, my_row >= my_col), jnp.logical_not(is_helper))

    @pl.when(early)
    def _():
        to_helper(0).start()

    @pl.when(is_helper)
    def _():
        for a in range(row_tiles):
            local(x_ref.at[a], tiles.at[own(a)], in_sem.at[own(a)]).start()

    @pl.when(jnp.logical_and(relayed, jnp.logical_not(first)))
    def _():
        to_relay(1).start()

    for p in range(3):

        @pl.when(relays[p])
        def _(p=p):
            settle(relay.at[p], relay_in.at[p])
            onward(p).start()

    late = jnp.logical_and(
        second, jnp.logical_or(jnp.logical_and(my_row == 2, my_col < 4), jnp.logical_and(my_row < 2, jnp.logical_not(far)))
    )

    @pl.when(late)
    def _():
        pl.semaphore_wait(go_sem, 1)

    end = jnp.logical_or(late, jnp.logical_and(my_row == root_row, jnp.logical_not(is_helper)))

    @pl.when(end)
    def _():
        to_helper(1).start()

    def arrive(slot):
        settle(tiles.at[slot], in_sem.at[slot])

    def deliver(slot, a, row, col):
        return remote(tiles.at[slot], o_ref.at[a], out_sem.at[slot], land_sem.at[a], (row, col))

    def hand(i, j):
        slot = i * steps + j
        return remote(tiles.at[slot], tiles.at[slot], out_sem.at[slot], in_sem.at[slot], via(i, j))

    def send(i, k):
        slot = i * steps + k
        row, a = lax.rem(i, num_row), i // num_row
        home = jnp.logical_and(my_row == row, my_col == k)

        @pl.when(home)
        def _():
            local(tiles.at[slot], o_ref.at[a], out_sem.at[slot]).start()

        through = jnp.zeros((), jnp.bool_)
        for p, q in PASSED:
            here = jnp.logical_and(i == p, k == q)
            through = jnp.logical_or(through, here)

            @pl.when(here)
            def _(p=p, q=q):
                hand(p, q).start()

        @pl.when(jnp.logical_not(jnp.logical_or(home, through)))
        def _():
            deliver(slot, a, row, k).start()

    def inv_copy(k, sem, device):
        return remote(inverse.at[k], inverse.at[k], sem, inv_in.at[k], device)

    def side_copy(k):
        return remote(tiles.at[(k + 1) * steps + k], beside.at[k], side_out.at[k], side_in.at[k], helper)

    rows = lax.broadcasted_iota(jnp.int32, (width, width), 0)
    cols = lax.broadcasted_iota(jnp.int32, (width, width), 1)

    def scales():
        only = jnp.where(rows == cols, work[...], 0.0)
        along = jnp.sum(only, axis=0, keepdims=True)
        down = jnp.sum(only, axis=1, keepdims=True)
        return along, down, lax.rsqrt(along), lax.rsqrt(down)

    def factor_of(along, down, scale_row, scale_col):
        upper = jnp.where(cols // SUBS > rows // SUBS, work[...] * (along * scale_row), 0.0)
        wide = jnp.concatenate([corner[...]] * (width // LANES), 1)
        near = jnp.logical_and(cols // SUBS == rows // SUBS, cols <= rows)
        return upper.T + jnp.where(near, wide * (down * scale_col), 0.0)

    def first_part(start):
        span = pl.ds(2 * start, 2 * PANEL)
        return remote(
            inverse.at[0, span], inverse.at[0, span], first_out.at[start // PANEL], first_in.at[start // PANEL], chief
        )

    first_waits = 3

    @pl.when(first)
    def _():
        work[...] = load(x_ref.at[0])
        along, down, scale_row, scale_col = scales()
        work[...] = work[...] * scale_row * scale_col
        def after(start):
            if start == 0:
                pl.semaphore_wait(barrier, first_waits)
            span = pl.ds(start, PANEL)
            kept = jnp.where(cols[:PANEL] <= rows[:PANEL] + start, work[span, :], 0.0)
            for h in range(width // LANES):
                inverse[0, pl.ds(2 * start + h, PANEL, stride=2), :] = kept[:, h * LANES : (h + 1) * LANES]
            first_part(start).start()

        factor_tile(work, corner, scale_row, width, after)
        to_relay(1).start()
        store(o_ref.at[0], factor_of(along, down, scale_row, scale_col))
        for start in range(0, width, PANEL):
            first_part(start).wait_send()

    @pl.when(is_chief)
    def _():
        def step(k, carry):
            slot = k * steps + k

            @pl.when(k == 1)
            def _():
                for start in range(0, width, PANEL):
                    first_part(start).wait_recv()
                inv_copy(0, inv_out.at[0], helper).start()
                for q in range(2, 4):
                    signal(go_sem, (0, q))
                inv_high[0], inv_low[0] = split(load(inverse.at[0]))

            @pl.when(k == 2)
            def _():
                for q in range(2, 4):
                    signal(go_sem, (1, q))

            left = slot - 1
            arrive(left)
            a_high, a_low = split(load(tiles.at[left]))
            solved = dot3(a_high, a_low, inv_high[0], inv_low[0])
            store(tiles.at[left], solved)
            own_high[...], own_low[...] = split(solved)

            @pl.when(k < steps - 1)
            def _():
                side_copy(k - 1).start()

            send(k, k - 1)

            arrive(slot)

            work[...] = load(tiles.at[slot])

            work[...] -= dot3(own_high[...], own_low[...], own_high[...], own_low[...])

            along, down, scale_row, scale_col = scales()
            work[...] = work[...] * scale_row * scale_col
            factor_tile(work, corner, scale_row, width)

            @pl.when(k < steps - 1)
            def _():
                found = jnp.where(cols <= rows, work[...], 0.0)
                store(inverse.at[k], found)
                inv_high[0], inv_low[0] = split(found)

            @pl.when(k < steps - 2)
            def _():
                inv_copy(k, inv_out.at[k], helper).start()

            store(tiles.at[slot], factor_of(along, down, scale_row, scale_col))
            send(k, k)
            return carry

        lax.fori_loop(1, steps, step, 0)

        def finish(k, carry):
            settle(tiles.at[k * steps + k], out_sem.at[k * steps + k])
            settle(tiles.at[k * steps + k - 1], out_sem.at[k * steps + k - 1])

            @pl.when(k < steps - 1)
            def _():
                settle(beside.at[k - 1], side_out.at[k - 1])

            @pl.when(k < steps - 2)
            def _():
                settle(inverse.at[k], inv_out.at[k])

            return carry

        lax.fori_loop(1, steps, finish, 0)
        settle(inverse.at[0], inv_out.at[0])

    def block(i):
        return pl.ds(pl.multiple_of(i * width, width), width)

    @pl.when(is_helper)
    def _():
        def row(i, carry):
            def whole(j, carry):
                arrive(i * steps + j)
                return carry

            lax.fori_loop(0, i + 1, whole, 0)

            @pl.when(i == 2)
            def _():
                for q in range(4):
                    signal(go_sem, (2, q))

            def stage(k, carry):
                @pl.when(k == i - 2)
                def _():
                    settle(inverse.at[k], inv_in.at[k])
                    inv_high[k], inv_low[k] = split(load(inverse.at[k]))
                    settle(beside.at[k], side_in.at[k])
                    high[block(k + 1), block(k)], low[block(k + 1), block(k)] = split(load(beside.at[k]))

                spot = i * steps + k
                a_high, a_low = split(load(tiles.at[spot]))
                solved = dot3(a_high, a_low, inv_high[k], inv_low[k])
                store(tiles.at[spot], solved)
                high[block(i), block(k)], low[block(i), block(k)] = split(solved)
                send(i, k)

                def some(j, size):
                    span = pl.ds(pl.multiple_of(j * width, width), size * width)
                    update = dot3(
                        high[block(i), block(k)], low[block(i), block(k)], high[span, block(k)], low[span, block(k)]
                    )
                    for t in range(size):
                        slot = i * steps + j + t
                        part = update[:, t * width : (t + 1) * width]
                        store(tiles.at[slot], load(tiles.at[slot]) - part)

                def three(q, carry):
                    some(k + 1 + 3 * q, 3)
                    return carry

                lax.fori_loop(0, (i - k) // 3, three, 0)
                for rest in (1, 2):

                    @pl.when(lax.rem(i - k, 3) == rest)
                    def _(rest=rest):
                        some(i + 1 - rest, rest)

                return carry

            lax.fori_loop(0, i - 1, stage, 0)
            for j in (i - 1, i):
                slot = i * steps + j
                remote(tiles.at[slot], tiles.at[slot], pass_sem.at[slot], in_sem.at[slot], chief).start()
            return carry

        lax.fori_loop(2, steps, row, 0)

        def finish(i, carry):
            def each(k, carry):
                settle(tiles.at[i * steps + k], out_sem.at[i * steps + k])
                return carry

            lax.fori_loop(0, i - 1, each, 0)
            for j in (i - 1, i):
                settle(tiles.at[i * steps + j], pass_sem.at[i * steps + j])
            return carry

        lax.fori_loop(2, steps, finish, 0)

    def onto(i, j):
        return deliver(i * steps + j, i // num_row, i % num_row, j)

    for i, j in PASSED:

        @pl.when(at(*via(i, j)))
        def _(i=i, j=j):
            arrive(i * steps + j)
            onto(i, j).start()

    for i, j in PASSED:

        @pl.when(at(*via(i, j)))
        def _(i=i, j=j):
            onto(i, j).wait_send()

    @pl.when(at(1, 1))
    def _():
        for p in range(2):
            half_in(p).wait_send()

    @pl.when(at(root_row, 1))
    def _():
        for p in range(2):
            half_on(p).wait_send()

    sent = [early, jnp.logical_or(relayed, end)]
    for a in range(row_tiles):

        @pl.when(sent[a])
        def _(a=a):
            to_helper(a).wait_send()

        i = a * num_row + my_row
        diagonal = jnp.logical_and(is_chief, i == my_col)
        below = jnp.logical_and(is_helper, i >= my_col + 2)
        mine = jnp.logical_or(jnp.logical_or(below, diagonal), jnp.logical_and(first, a == 0))

        @pl.when(jnp.logical_and(i >= my_col, jnp.logical_not(mine)))
        def _(a=a):
            settle(o_ref.at[a], land_sem.at[a])

    for p in range(3):

        @pl.when(relays[p])
        def _(p=p):
            onward(p).wait_send()


def on_root(matrix):
    row_tiles = matrix.shape[0]
    width = matrix.shape[2]
    num_row, num_col = lax.axis_size("row"), lax.axis_size("col")
    order = STEPS * width
    tall = width * width // LANES
    local = matrix.reshape(row_tiles, tall, LANES)
    slots = STEPS * STEPS
    sem = pltpu.SemaphoreType.DMA
    out = pl.pallas_call(
        functools.partial(kernel, (STEPS, num_row, num_col)),
        out_shape=jax.ShapeDtypeStruct(local.shape, jnp.float32),
        in_specs=[pl.BlockSpec(memory_space=pltpu.VMEM)],
        out_specs=pl.BlockSpec(memory_space=pltpu.VMEM),
        scratch_shapes=[
            pltpu.VMEM((slots, tall, LANES), jnp.float32),
            pltpu.VMEM((STEPS, tall, LANES), jnp.float32),
            pltpu.VMEM((STEPS, tall, LANES), jnp.float32),
            pltpu.VMEM((3, tall, LANES), jnp.float32),
            pltpu.VMEM((order, order), jnp.bfloat16),
            pltpu.VMEM((order, order), jnp.bfloat16),
            pltpu.VMEM((width, width), jnp.bfloat16),
            pltpu.VMEM((width, width), jnp.bfloat16),
            pltpu.VMEM((STEPS, width, width), jnp.bfloat16),
            pltpu.VMEM((STEPS, width, width), jnp.bfloat16),
            pltpu.VMEM((width, width), jnp.float32),
            pltpu.VMEM((width, LANES), jnp.float32),
            sem((slots,)), sem((slots,)), sem((slots,)), sem((STEPS,)), sem((STEPS,)),
            sem((width // PANEL,)), sem((width // PANEL,)), sem((STEPS,)),
            sem((STEPS,)), sem((row_tiles,)), sem((row_tiles,)), sem((3,)), sem((3,)),
            sem((3, 2)),
            pltpu.SemaphoreType.REGULAR,
        ],
        compiler_params=pltpu.CompilerParams(collective_id=0, has_side_effects=True, vmem_limit_bytes=56 * 2**20),
    )(local)
    rows = jnp.arange(row_tiles) * num_row + lax.axis_index("row")
    kept = jnp.where((rows >= lax.axis_index("col"))[:, None, None], out, 0.0)
    return kept.reshape(matrix.shape)


def broadcast(value, axis, source):
    kept = jnp.where(lax.axis_index(axis) == source, value, 0).astype(value.dtype)
    return lax.psum(kept, axis)


def solve_panel(factor, column):
    width = column.shape[1]
    inverse = jax.scipy.linalg.solve_triangular(
        factor, jnp.eye(width, dtype=jnp.float32), lower=True
    )
    solved = jnp.einsum("ts,ars->art", inverse, column, precision=lax.Precision.HIGHEST)
    return solved


def stepwise(matrix):
    row_tiles = matrix.shape[0]
    width = matrix.shape[2]
    col_tiles = matrix.shape[3]
    tile_grid = matrix.reshape(row_tiles, width, col_tiles, width)
    num_row = lax.axis_size("row")
    num_col = lax.axis_size("col")
    my_row = lax.axis_index("row")
    my_col = lax.axis_index("col")
    rows_global = jnp.arange(row_tiles, dtype=jnp.int32) * num_row + my_row
    ratio = num_col // num_row
    for k in range(STEPS):
        lead_row = k % num_row
        lead_col = k % num_col
        local_row = k // num_row
        local_col = k // num_col
        column = tile_grid[:, :, local_col, :]
        candidate = tile_grid[local_row, :, local_col, :]
        keep = (rows_global > k)[:, None, None]
        diag_tile = broadcast(candidate, "row", lead_row)
        factor = jnp.linalg.cholesky(diag_tile)
        local_panel = jnp.where(keep, solve_panel(factor, column), 0.0)
        panel_rows = broadcast(local_panel, "col", lead_col)
        grouped = panel_rows.reshape(col_tiles, ratio, width, width)
        chosen = lax.dynamic_index_in_dim(grouped, my_col // num_row, 1, keepdims=False)
        panel_cols = broadcast(chosen, "row", my_col % num_row)
        update = jnp.einsum(
            "art,bst->arbs", panel_rows, panel_cols, precision=lax.Precision.HIGHEST
        )
        tile_grid = tile_grid - update
        diagonal_part = jnp.where((rows_global == k)[:, None, None], factor[None], 0.0)
        new_column = panel_rows + diagonal_part
        old_column = tile_grid[:, :, local_col, :]
        tile_grid = tile_grid.at[:, :, local_col, :].set(
            jnp.where(my_col == lead_col, new_column, old_column)
        )
    return tile_grid.reshape(matrix.shape)


def on_device(matrix):
    row_tiles, _, _, col_tiles = matrix.shape[:4]
    whole = row_tiles == 2 and 2 * lax.axis_size("row") == STEPS and lax.axis_size("col") == STEPS and col_tiles == 1
    return on_root(matrix) if whole else stepwise(matrix)


def solution(mesh):
    placed = (P(None, "row", None, None, "col", None),)
    return jax.shard_map(
        on_device,
        mesh=mesh,
        in_specs=placed,
        out_specs=P(None, "row", None, None, "col", None),
        check_vma=False,
    )
```

```python
import functools

import jax
import jax.numpy as jnp
from jax import lax
from jax.experimental import pallas as pl
from jax.experimental.pallas import tpu as pltpu
from jax.sharding import PartitionSpec as P

STEPS = 8
LANES = 128
SUBS = 8
PANEL = 64
BLOCK = 16
SHAPE = (SUBS, LANES)
MESH = pl.DeviceIdType.MESH
PASSED = ((4, 0), (4, 1), (4, 4), (5, 4), (5, 5), (6, 5), (6, 6))
NT = (((1,), (1,)), ((), ()))
TN = (((0,), (0,)), ((), ()))


def split(value):
    high = value.astype(jnp.bfloat16)
    low = (value - high.astype(jnp.float32)).astype(jnp.bfloat16)
    return high, low


def dot3(a_high, a_low, b_high, b_low):
    def one(a, b):
        return lax.dot_general(a, b, NT, preferred_element_type=jnp.float32)

    return one(a_high, b_high) + (one(a_high, b_low) + one(a_low, b_high))


def spread(value, at):
    return jnp.broadcast_to(value[at:at+1,:], SHAPE)

def factor_panel(work, diag, unit, width, start, after):
    groups = PANEL//SUBS
    chunks = width//LANES
    sub = lax.broadcasted_iota(jnp.int32, SHAPE, 0)
    lane = lax.broadcasted_iota(jnp.int32, SHAPE, 1)
    rows = [[work[start+g*SUBS:start+(g+1)*SUBS, h*LANES:(h+1)*LANES] for h in range(chunks)] for g in range(groups)]
    per = BLOCK//SUBS
    for b in range(PANEL//BLOCK):
        home = b*per
        l0 = start + b*BLOCK
        hc, off = l0//LANES, l0%LANES
        def pick(g, t):
            return jnp.take_along_axis(rows[g][hc], jnp.full(SHAPE, off+t, jnp.int32), axis=1)
        near = min(home+per, groups)
        far = list(range(near, groups))
        cols = [{g: pick(g,t) for g in range(home + t//SUBS, near)} for t in range(BLOCK)]
        fcols = [{g: pick(g,t) for g in far} for t in range(SUBS)] + [{}]*SUBS
        scales = {g: jnp.ones(SHAPE, jnp.float32) for g in range(home, home+per)}
        lower = {g: jnp.zeros(SHAPE, jnp.float32) for g in range(home, home+per)}
        for t in range(0, BLOCK, 2):
            top = home + t//SUBS
            r = t%SUBS
            if t == SUBS and far:
                fcols = [None]*SUBS + [{g: pick(g,SUBS+q) for g in far} for q in range(SUBS)]
            if r == 0:
                inside = jnp.logical_and(lane>=off+t, lane<off+t+SUBS)
                eye = jnp.where(lane == off+t+sub, unit[hc], 0.0)
                for g in range(top, groups):
                    rows[g][hc] = jnp.where(inside, eye if g == top else 0.0, rows[g][hc])
            x, y = dict(cols[t]), dict(cols[t+1])
            fx, fy = fcols[t], fcols[t+1]
            a, bb, c = spread(x[top], r), spread(x[top], r+1), spread(y[top], r+1)
            det = a*c - bb*bb
            ra = lax.rsqrt(a)
            rd = lax.rsqrt(a*det)
            ia, iad = ra*ra, rd*rd
            u = {g: y[g]*a - x[g]*bb for g in y}
            fu = {g: fy[g]*a - fx[g]*bb for g in far}
            mx = {g: x[g]*ia for g in x}
            mu = {g: u[g]*iad for g in u}
            fmx = {g: fx[g]*ia for g in far}
            fmu = {g: fu[g]*iad for g in far}
            for s in range(t+2, BLOCK):
                gs, q = home + s//SUBS, s%SUBS
                xs, us = spread(x[gs], q), spread(u[gs], q)
                for g in cols[s]:
                    if s < t+4 and g == gs:
                        cols[s][g] = (cols[s][g] - xs*mx[g]) - (us*u[g])*iad
                    else:
                        cols[s][g] = cols[s][g] - xs*mx[g] - us*mu[g]
                if s < SUBS or t >= SUBS:
                    for g in far:
                        fcols[s][g] = fcols[s][g] - xs*fmx[g] - us*fmu[g]
            for g in [top]:
                lower[g] = jnp.where(lane==off+t, x[g]*ra, jnp.where(lane==off+t+1, u[g]*rd, lower[g]))
            scales[top] = jnp.where(sub==r, ra, jnp.where(sub==r+1, a*rd, scales[top]))
            mx[top] = jnp.where(sub>r, mx[top], 0.0)
            mu[top] = jnp.where(sub>r+1, mu[top], 0.0)
            for h in range(chunks):
                p0, q1 = spread(rows[top][h], r), spread(rows[top][h], r+1)
                p1 = q1*a - p0*bb
                for g in range(top, groups):
                    m, n = (fmx[g], fmu[g]) if g in far else (mx[g], mu[g])
                    rows[g][h] = rows[g][h] - m*p0 - n*p1
            if r == SUBS-2:
                rows[top] = [v*scales[top] for v in rows[top]]
        for g in range(home, home+per):
            diag[start+g*SUBS:start+(g+1)*SUBS, :] = lower[g]
    for g in range(groups):
        for h in range(chunks):
            work[start+g*SUBS:start+(g+1)*SUBS, h*LANES:(h+1)*LANES] = rows[g][h]
    stop = start+PANEL
    after(start)
    if stop == width: return
    hc = start//LANES
    for g in range(groups):
        gap = jnp.logical_and(lane>=start%LANES+(g+1)*SUBS, lane<start%LANES+PANEL)
        rows[g][hc] = jnp.where(gap, 0.0, rows[g][hc])
    whole = jnp.concatenate([jnp.concatenate(r,1) for r in rows],0)
    high, low = split(whole)
    base = stop//LANES*LANES
    lh, ll = high[:, base:], low[:, base:]
    update = lax.dot_general(jnp.concatenate([lh,lh,ll],0), jnp.concatenate([high,low,high],0), TN, preferred_element_type=jnp.float32)
    lanes = lax.broadcasted_iota(jnp.int32, (width-stop, width), 1)
    old = jnp.where(jnp.logical_and(lanes >= start, lanes < stop), 0.0, work[stop:, :])
    work[stop:, :] = old - update[stop-base:, :]

def factor_tile(work, diag, scale_row, width, after=lambda start: None):
    chunks = width//LANES
    unit = [jnp.broadcast_to(scale_row[:, h*LANES:(h+1)*LANES], SHAPE) for h in range(chunks)]
    for start in range(0, width, PANEL):
        factor_panel(work, diag, unit, width, start, after)


def load(ref):
    half = ref.shape[0] // 2
    return jnp.concatenate([ref[pl.ds(h, half, stride=2), :] for h in range(2)], 1)


def store(ref, value):
    half = ref.shape[0] // 2
    for h in range(2):
        ref[pl.ds(h, half, stride=2), :] = value[:, h * LANES : (h + 1) * LANES]


def kernel(
    dims, x_ref, o_ref, tiles, inverse, beside, relay, high, low, own_high, own_low, inv_high, inv_low, work, corner,
    in_sem, out_sem, pass_sem, inv_in, inv_out, first_in, first_out, side_in, side_out, send_sem, land_sem, relay_in, relay_out,
    half_sem, go_sem,
):
    steps, num_row, num_col = dims
    row_tiles = x_ref.shape[0]
    width = work.shape[0]
    my_row, my_col = lax.axis_index("row"), lax.axis_index("col")
    root_row = num_row - 1
    chief, helper = (root_row, 3), (root_row, 2)
    first = jnp.logical_and(my_row == 0, my_col == 0)
    is_chief = jnp.logical_and(my_row == chief[0], my_col == chief[1])
    is_helper = jnp.logical_and(my_row == helper[0], my_col == helper[1])
    count = num_row * num_col
    me = my_row * num_col + my_col
    barrier = pltpu.get_barrier_semaphore()
    far = jnp.logical_or(my_col < 2, my_col > 3)

    def remote(src, dst, send, recv, device):
        return pltpu.make_async_remote_copy(
            src_ref=src, dst_ref=dst, send_sem=send, recv_sem=recv, device_id=device, device_id_type=MESH
        )

    def local(src, dst, sem):
        return pltpu.make_async_copy(src, dst, sem)

    def settle(ref, sem):
        pltpu.make_async_copy(ref, ref, sem).wait()

    def own(a):
        return (a * num_row + my_row) * steps + my_col

    def to_chief(a):
        return remote(x_ref.at[a], tiles.at[own(a)], send_sem.at[a], in_sem.at[own(a)], chief)

    def to_helper(a):
        return remote(x_ref.at[a], tiles.at[own(a)], send_sem.at[a], in_sem.at[own(a)], helper)

    def to_relay(a):
        return remote(x_ref.at[a], relay.at[my_row], send_sem.at[a], relay_in.at[my_row], (root_row, my_col))

    def onward(p):
        slot = (num_row + p) * steps + my_col
        return remote(relay.at[p], tiles.at[slot], relay_out.at[p], in_sem.at[slot], helper)

    def signal(sem, device):
        pl.semaphore_signal(sem, inc=1, device_id=device, device_id_type=MESH)

    def via(i, j):
        return max(i % num_row, 1), 2 + j % 2

    def at(row, col):
        return jnp.logical_and(my_row == row, my_col == col)

    second = num_row + my_row >= my_col
    relayed = jnp.logical_and(jnp.logical_and(far, second), my_row < jnp.where(my_col > 3, 3, 2))
    at_relay = jnp.logical_and(my_row == root_row, far)
    relays = [jnp.logical_and(at_relay, num_row + p >= my_col) for p in range(2)]
    relays.append(jnp.logical_and(at_relay, jnp.logical_and(my_col > 3, num_row + 2 >= my_col)))

    @pl.when(jnp.logical_not(is_chief))
    def _():
        signal(barrier, chief)

    @pl.when(jnp.logical_not(is_helper))
    def _():
        signal(barrier, helper)

    for p in range(3):

        @pl.when(relays[p])
        def _(p=p):
            signal(barrier, (p, my_col))

    for i, j in PASSED:

        @pl.when(at(i % num_row, j))
        def _(i=i, j=j):
            signal(barrier, via(i, j))

    @pl.when(at(0, 1))
    def _():
        signal(barrier, (root_row, 1))

    @pl.when(jnp.logical_or(is_chief, is_helper))
    def _():
        def greet(d, carry):
            signal(barrier, (lax.rem(d, num_row), d // num_row))
            return carry

        low_end, high_end = helper[1] * num_row + helper[0], chief[1] * num_row + chief[0]
        lax.fori_loop(0, low_end, greet, 0)
        lax.fori_loop(low_end + 1, high_end, greet, 0)
        lax.fori_loop(high_end + 1, count, greet, 0)
        pl.semaphore_wait(barrier, count - 1)

    @pl.when(jnp.logical_not(jnp.logical_or(first, jnp.logical_or(is_chief, is_helper))))
    def _():
        expected = jnp.where(jnp.logical_or(relayed, at(root_row, 1)), 3, 2)
        for i, j in PASSED:
            expected += jnp.where(at(*via(i, j)), 1, 0)
        pl.semaphore_wait(barrier, expected)

    tall = x_ref.shape[1]
    corner_slot = steps + 1

    def half_in(p):
        span = pl.ds(p * (tall // 2), tall // 2)
        return remote(x_ref.at[0, span], relay.at[2, span], half_sem.at[0, p], half_sem.at[1, p], (root_row, 1))

    def half_on(p):
        span = pl.ds(p * (tall // 2), tall // 2)
        return remote(
            relay.at[2, span], tiles.at[corner_slot, span], half_sem.at[2, p], in_sem.at[corner_slot], chief
        )

    begin = at(1, 0)

    @pl.when(begin)
    def _():
        to_chief(0).start()
        to_chief(0).wait_send()

    @pl.when(at(1, 1))
    def _():
        for p in range(2):
            half_in(p).start()

    @pl.when(at(root_row, 1))
    def _():
        for p in range(2):
            half_in(p).wait_recv()
            half_on(p).start()
        signal(go_sem, (0, 1))

    @pl.when(at(0, 1))
    def _():
        pl.semaphore_wait(go_sem, 1)

    early = jnp.logical_and(jnp.logical_and(my_row >= 2, my_row >= my_col), jnp.logical_not(is_helper))

    @pl.when(early)
    def _():
        to_helper(0).start()

    @pl.when(is_helper)
    def _():
        for a in range(row_tiles):
            local(x_ref.at[a], tiles.at[own(a)], in_sem.at[own(a)]).start()

    @pl.when(jnp.logical_and(relayed, jnp.logical_not(first)))
    def _():
        to_relay(1).start()

    for p in range(3):

        @pl.when(relays[p])
        def _(p=p):
            settle(relay.at[p], relay_in.at[p])
            onward(p).start()

    late = jnp.logical_and(
        second, jnp.logical_or(jnp.logical_and(my_row == 2, my_col < 4), jnp.logical_and(my_row < 2, jnp.logical_not(far)))
    )

    @pl.when(late)
    def _():
        pl.semaphore_wait(go_sem, 1)

    end = jnp.logical_or(late, jnp.logical_and(my_row == root_row, jnp.logical_not(is_helper)))

    @pl.when(end)
    def _():
        to_helper(1).start()

    def arrive(slot):
        settle(tiles.at[slot], in_sem.at[slot])

    def deliver(slot, a, row, col):
        return remote(tiles.at[slot], o_ref.at[a], out_sem.at[slot], land_sem.at[a], (row, col))

    def hand(i, j):
        slot = i * steps + j
        return remote(tiles.at[slot], tiles.at[slot], out_sem.at[slot], in_sem.at[slot], via(i, j))

    def send(i, k):
        slot = i * steps + k
        row, a = lax.rem(i, num_row), i // num_row
        home = jnp.logical_and(my_row == row, my_col == k)

        @pl.when(home)
        def _():
            local(tiles.at[slot], o_ref.at[a], out_sem.at[slot]).start()

        through = jnp.zeros((), jnp.bool_)
        for p, q in PASSED:
            here = jnp.logical_and(i == p, k == q)
            through = jnp.logical_or(through, here)

            @pl.when(here)
            def _(p=p, q=q):
                hand(p, q).start()

        @pl.when(jnp.logical_not(jnp.logical_or(home, through)))
        def _():
            deliver(slot, a, row, k).start()

    def inv_copy(k, sem, device):
        return remote(inverse.at[k], inverse.at[k], sem, inv_in.at[k], device)

    def side_copy(k):
        return remote(tiles.at[(k + 1) * steps + k], beside.at[k], side_out.at[k], side_in.at[k], helper)

    rows = lax.broadcasted_iota(jnp.int32, (width, width), 0)
    cols = lax.broadcasted_iota(jnp.int32, (width, width), 1)

    def scales():
        only = jnp.where(rows == cols, work[...], 0.0)
        along = jnp.sum(only, axis=0, keepdims=True)
        down = jnp.sum(only, axis=1, keepdims=True)
        return along, down, lax.rsqrt(along), lax.rsqrt(down)

    def factor_of(along, down, scale_row, scale_col):
        upper = jnp.where(cols // SUBS > rows // SUBS, work[...] * (along * scale_row), 0.0)
        wide = jnp.concatenate([corner[...]] * (width // LANES), 1)
        near = jnp.logical_and(cols // SUBS == rows // SUBS, cols <= rows)
        return upper.T + jnp.where(near, wide * (down * scale_col), 0.0)

    def first_part(start):
        span = pl.ds(2 * start, 2 * PANEL)
        return remote(
            inverse.at[0, span], inverse.at[0, span], first_out.at[start // PANEL], first_in.at[start // PANEL], chief
        )

    first_waits = 3

    @pl.when(first)
    def _():
        work[...] = load(x_ref.at[0])
        along, down, scale_row, scale_col = scales()
        work[...] = work[...] * scale_row * scale_col
        def after(start):
            if start == 0:
                pl.semaphore_wait(barrier, first_waits)
            span = pl.ds(start, PANEL)
            kept = jnp.where(cols[:PANEL] <= rows[:PANEL] + start, work[span, :], 0.0)
            for h in range(width // LANES):
                inverse[0, pl.ds(2 * start + h, PANEL, stride=2), :] = kept[:, h * LANES : (h + 1) * LANES]
            first_part(start).start()

        factor_tile(work, corner, scale_row, width, after)
        to_relay(1).start()
        store(o_ref.at[0], factor_of(along, down, scale_row, scale_col))
        for start in range(0, width, PANEL):
            first_part(start).wait_send()

    @pl.when(is_chief)
    def _():
        def step(k, carry):
            slot = k * steps + k

            @pl.when(k == 1)
            def _():
                for start in range(0, width, PANEL):
                    first_part(start).wait_recv()
                inv_copy(0, inv_out.at[0], helper).start()
                for q in range(2, 4):
                    signal(go_sem, (0, q))
                inv_high[0], inv_low[0] = split(load(inverse.at[0]))

            @pl.when(k == 2)
            def _():
                for q in range(2, 4):
                    signal(go_sem, (1, q))

            left = slot - 1
            arrive(left)
            a_high, a_low = split(load(tiles.at[left]))
            solved = dot3(a_high, a_low, inv_high[0], inv_low[0])
            store(tiles.at[left], solved)
            own_high[...], own_low[...] = split(solved)

            @pl.when(k < steps - 1)
            def _():
                side_copy(k - 1).start()

            send(k, k - 1)

            arrive(slot)

            work[...] = load(tiles.at[slot])

            work[...] -= dot3(own_high[...], own_low[...], own_high[...], own_low[...])

            along, down, scale_row, scale_col = scales()
            work[...] = work[...] * scale_row * scale_col
            factor_tile(work, corner, scale_row, width)

            @pl.when(k < steps - 1)
            def _():
                found = jnp.where(cols <= rows, work[...], 0.0)
                store(inverse.at[k], found)
                inv_high[0], inv_low[0] = split(found)

            @pl.when(k < steps - 2)
            def _():
                inv_copy(k, inv_out.at[k], helper).start()

            store(tiles.at[slot], factor_of(along, down, scale_row, scale_col))
            send(k, k)
            return carry

        lax.fori_loop(1, steps, step, 0)

        def finish(k, carry):
            settle(tiles.at[k * steps + k], out_sem.at[k * steps + k])
            settle(tiles.at[k * steps + k - 1], out_sem.at[k * steps + k - 1])

            @pl.when(k < steps - 1)
            def _():
                settle(beside.at[k - 1], side_out.at[k - 1])

            @pl.when(k < steps - 2)
            def _():
                settle(inverse.at[k], inv_out.at[k])

            return carry

        lax.fori_loop(1, steps, finish, 0)
        settle(inverse.at[0], inv_out.at[0])

    def block(i):
        return pl.ds(pl.multiple_of(i * width, width), width)

    @pl.when(is_helper)
    def _():
        def row(i, carry):
            def whole(j, carry):
                arrive(i * steps + j)
                return carry

            lax.fori_loop(0, i + 1, whole, 0)

            @pl.when(i == 2)
            def _():
                for q in range(4):
                    signal(go_sem, (2, q))

            def stage(k, carry):
                @pl.when(k == i - 2)
                def _():
                    settle(inverse.at[k], inv_in.at[k])
                    inv_high[k], inv_low[k] = split(load(inverse.at[k]))
                    settle(beside.at[k], side_in.at[k])
                    high[block(k + 1), block(k)], low[block(k + 1), block(k)] = split(load(beside.at[k]))

                spot = i * steps + k
                a_high, a_low = split(load(tiles.at[spot]))
                solved = dot3(a_high, a_low, inv_high[k], inv_low[k])
                store(tiles.at[spot], solved)
                high[block(i), block(k)], low[block(i), block(k)] = split(solved)
                send(i, k)

                def some(j, size):
                    span = pl.ds(pl.multiple_of(j * width, width), size * width)
                    update = dot3(
                        high[block(i), block(k)], low[block(i), block(k)], high[span, block(k)], low[span, block(k)]
                    )
                    for t in range(size):
                        slot = i * steps + j + t
                        part = update[:, t * width : (t + 1) * width]
                        store(tiles.at[slot], load(tiles.at[slot]) - part)

                def four(q, carry):
                    some(k + 1 + 4 * q, 4)
                    return carry

                lax.fori_loop(0, (i - k) // 4, four, 0)
                for rest in (1, 2, 3):

                    @pl.when(lax.rem(i - k, 4) == rest)
                    def _(rest=rest):
                        some(i + 1 - rest, rest)

                return carry

            lax.fori_loop(0, i - 1, stage, 0)
            for j in (i - 1, i):
                slot = i * steps + j
                remote(tiles.at[slot], tiles.at[slot], pass_sem.at[slot], in_sem.at[slot], chief).start()
            return carry

        lax.fori_loop(2, steps, row, 0)

        def finish(i, carry):
            def each(k, carry):
                settle(tiles.at[i * steps + k], out_sem.at[i * steps + k])
                return carry

            lax.fori_loop(0, i - 1, each, 0)
            for j in (i - 1, i):
                settle(tiles.at[i * steps + j], pass_sem.at[i * steps + j])
            return carry

        lax.fori_loop(2, steps, finish, 0)

    def onto(i, j):
        return deliver(i * steps + j, i // num_row, i % num_row, j)

    for i, j in PASSED:

        @pl.when(at(*via(i, j)))
        def _(i=i, j=j):
            arrive(i * steps + j)
            onto(i, j).start()

    for i, j in PASSED:

        @pl.when(at(*via(i, j)))
        def _(i=i, j=j):
            onto(i, j).wait_send()

    @pl.when(at(1, 1))
    def _():
        for p in range(2):
            half_in(p).wait_send()

    @pl.when(at(root_row, 1))
    def _():
        for p in range(2):
            half_on(p).wait_send()

    sent = [early, jnp.logical_or(relayed, end)]
    for a in range(row_tiles):

        @pl.when(sent[a])
        def _(a=a):
            to_helper(a).wait_send()

        i = a * num_row + my_row
        diagonal = jnp.logical_and(is_chief, i == my_col)
        below = jnp.logical_and(is_helper, i >= my_col + 2)
        mine = jnp.logical_or(jnp.logical_or(below, diagonal), jnp.logical_and(first, a == 0))

        @pl.when(jnp.logical_and(i >= my_col, jnp.logical_not(mine)))
        def _(a=a):
            settle(o_ref.at[a], land_sem.at[a])

    for p in range(3):

        @pl.when(relays[p])
        def _(p=p):
            onward(p).wait_send()


def on_root(matrix):
    row_tiles = matrix.shape[0]
    width = matrix.shape[2]
    num_row, num_col = lax.axis_size("row"), lax.axis_size("col")
    order = STEPS * width
    tall = width * width // LANES
    local = matrix.reshape(row_tiles, tall, LANES)
    slots = STEPS * STEPS
    sem = pltpu.SemaphoreType.DMA
    out = pl.pallas_call(
        functools.partial(kernel, (STEPS, num_row, num_col)),
        out_shape=jax.ShapeDtypeStruct(local.shape, jnp.float32),
        in_specs=[pl.BlockSpec(memory_space=pltpu.VMEM)],
        out_specs=pl.BlockSpec(memory_space=pltpu.VMEM),
        scratch_shapes=[
            pltpu.VMEM((slots, tall, LANES), jnp.float32),
            pltpu.VMEM((STEPS, tall, LANES), jnp.float32),
            pltpu.VMEM((STEPS, tall, LANES), jnp.float32),
            pltpu.VMEM((3, tall, LANES), jnp.float32),
            pltpu.VMEM((order, order), jnp.bfloat16),
            pltpu.VMEM((order, order), jnp.bfloat16),
            pltpu.VMEM((width, width), jnp.bfloat16),
            pltpu.VMEM((width, width), jnp.bfloat16),
            pltpu.VMEM((STEPS, width, width), jnp.bfloat16),
            pltpu.VMEM((STEPS, width, width), jnp.bfloat16),
            pltpu.VMEM((width, width), jnp.float32),
            pltpu.VMEM((width, LANES), jnp.float32),
            sem((slots,)), sem((slots,)), sem((slots,)), sem((STEPS,)), sem((STEPS,)),
            sem((width // PANEL,)), sem((width // PANEL,)), sem((STEPS,)),
            sem((STEPS,)), sem((row_tiles,)), sem((row_tiles,)), sem((3,)), sem((3,)),
            sem((3, 2)),
            pltpu.SemaphoreType.REGULAR,
        ],
        compiler_params=pltpu.CompilerParams(collective_id=0, has_side_effects=True, vmem_limit_bytes=56 * 2**20),
    )(local)
    rows = jnp.arange(row_tiles) * num_row + lax.axis_index("row")
    kept = jnp.where((rows >= lax.axis_index("col"))[:, None, None], out, 0.0)
    return kept.reshape(matrix.shape)


def broadcast(value, axis, source):
    kept = jnp.where(lax.axis_index(axis) == source, value, 0).astype(value.dtype)
    return lax.psum(kept, axis)


def solve_panel(factor, column):
    width = column.shape[1]
    inverse = jax.scipy.linalg.solve_triangular(
        factor, jnp.eye(width, dtype=jnp.float32), lower=True
    )
    solved = jnp.einsum("ts,ars->art", inverse, column, precision=lax.Precision.HIGHEST)
    return solved


def stepwise(matrix):
    row_tiles = matrix.shape[0]
    width = matrix.shape[2]
    col_tiles = matrix.shape[3]
    tile_grid = matrix.reshape(row_tiles, width, col_tiles, width)
    num_row = lax.axis_size("row")
    num_col = lax.axis_size("col")
    my_row = lax.axis_index("row")
    my_col = lax.axis_index("col")
    rows_global = jnp.arange(row_tiles, dtype=jnp.int32) * num_row + my_row
    ratio = num_col // num_row
    for k in range(STEPS):
        lead_row = k % num_row
        lead_col = k % num_col
        local_row = k // num_row
        local_col = k // num_col
        column = tile_grid[:, :, local_col, :]
        candidate = tile_grid[local_row, :, local_col, :]
        keep = (rows_global > k)[:, None, None]
        diag_tile = broadcast(candidate, "row", lead_row)
        factor = jnp.linalg.cholesky(diag_tile)
        local_panel = jnp.where(keep, solve_panel(factor, column), 0.0)
        panel_rows = broadcast(local_panel, "col", lead_col)
        grouped = panel_rows.reshape(col_tiles, ratio, width, width)
        chosen = lax.dynamic_index_in_dim(grouped, my_col // num_row, 1, keepdims=False)
        panel_cols = broadcast(chosen, "row", my_col % num_row)
        update = jnp.einsum(
            "art,bst->arbs", panel_rows, panel_cols, precision=lax.Precision.HIGHEST
        )
        tile_grid = tile_grid - update
        diagonal_part = jnp.where((rows_global == k)[:, None, None], factor[None], 0.0)
        new_column = panel_rows + diagonal_part
        old_column = tile_grid[:, :, local_col, :]
        tile_grid = tile_grid.at[:, :, local_col, :].set(
            jnp.where(my_col == lead_col, new_column, old_column)
        )
    return tile_grid.reshape(matrix.shape)


def on_device(matrix):
    row_tiles, _, _, col_tiles = matrix.shape[:4]
    whole = row_tiles == 2 and 2 * lax.axis_size("row") == STEPS and lax.axis_size("col") == STEPS and col_tiles == 1
    return on_root(matrix) if whole else stepwise(matrix)


def solution(mesh):
    placed = (P(None, "row", None, None, "col", None),)
    return jax.shard_map(
        on_device,
        mesh=mesh,
        in_specs=placed,
        out_specs=P(None, "row", None, None, "col", None),
        check_vma=False,
    )
```
